256 devices in a mesh: pair: 32 (over z, x), aux: 8 (over y, core).
Axes of the slice: x: 4, y: 4, z: 8, core: 2. Of those that a mesh axis runs over, the one named last changes fastest.
Arguments:
- integrals: bfloat16 [98304, 12288], P('pair', 'aux'), may hold values from -0.15625 to 0.15625
- energy_gaps: float32 [98304], P('pair'), may hold values from 0.3 to 3
- trial_vectors: float32 [98304, 64], P('pair'), may hold values from -160 to 160
Outputs:
- sigma_vectors: float32 [98304, 64], P(('pair', 'aux'))
- subspace: float32 [64, 64], replicated
- residuals: float32 [98304, 64], P(('pair', 'aux'))
- residual_norms: float32 [64], replicated
The draws below stay inside these ranges and needn't reach their ends.
All inputs are finite; a program needn't handle non-finite values.
Results may differ from the reference program's by a relative error of at most 0.0052.
Values may be sent and summed in bfloat16 or wider, within the bound.
No kernel may reach another device: no remote copies, remote signals or barrier semaphores. Data moves between devices by JAX's collectives and lax.ppermute only.
A program may use at most 64 MiB of HBM per device.

```python
import math
import jax
import jax.numpy as jnp
from jax import lax

NAUX = 12288
NVEC = 64
PAIRS = 98304


def draw_trial_vectors(key, part):
    key_entries = jax.random.fold_in(key, 11)
    key_rows = jax.random.fold_in(key, 12)
    key_columns = jax.random.fold_in(key, 13)
    positions = jnp.arange(PAIRS).astype(jnp.float32)
    growth = jnp.exp(jnp.log(3.0) * positions / PAIRS)
    row_scale = jnp.exp(jax.random.uniform(key_rows, (PAIRS,), jnp.float32, jnp.log(0.3), jnp.log(3.0)))
    entries = jnp.clip(jax.random.normal(key_entries, (PAIRS, NVEC), jnp.float32), -5.0, 5.0)
    column_scale = jnp.exp(jax.random.uniform(key_columns, (NVEC,), jnp.float32, jnp.log(0.3), jnp.log(3.0)))
    return (entries * (growth * row_scale)[:, None] * column_scale[None, :]).astype(jnp.float32)


def spiked(values, rng, source, target, blocks, factor):
    def block_of(dim):
        return (jnp.arange(values.shape[dim]) // (values.shape[dim] // blocks)).reshape((-1,) + (1,) * (values.ndim - 1 - dim))

    first = jax.random.permutation(rng, blocks)[block_of(target)]
    second = (block_of(target) + blocks // 2) % blocks
    return jnp.where((block_of(source) == first) | (block_of(source) == second), factor * values, values)


def block_levels(rng, extent, split, low, high):
    factor_of, own = 1.0, jax.random.fold_in(rng, 6)
    for dim, blocks in split:
        heights = jnp.exp(jax.random.uniform(jax.random.fold_in(own, dim), (blocks,), jnp.float32, low / len(split), high / len(split)))
        factor_of = factor_of * jnp.repeat(heights, extent[dim] // blocks).reshape([-1 if axis == dim else 1 for axis in range(len(extent))])
    return factor_of


def heavy_noise(rng, shape, spread, limit, pieces, heavy, held_as=jnp.bfloat16):
    values = spread * jax.random.normal(rng, shape, jnp.float32)
    if pieces:
        values = values * block_levels(rng, shape, pieces, -0.22, 0.18)
    return jnp.clip(spiked(values, jax.random.fold_in(rng, 3), *heavy), -limit, limit).astype(held_as)


def setup_inputs(seed: int = 0) -> dict:
    streams_of = jax.random.split(jax.random.key(seed), 4)
    return {
        "integrals": heavy_noise(streams_of[0], (PAIRS, NAUX), (1.0 / (PAIRS * NAUX) ** 0.25), 0.15625, ((0, 32), (1, 8)), (0, 1, 32, 2.75)),
        "energy_gaps": jnp.clip(jnp.exp(math.log(3.0) - 2.3025851 * jax.random.uniform(streams_of[1], (PAIRS,), jnp.float32) ** block_levels(streams_of[1], (PAIRS,), ((0, 32),), -0.2, 0.2)), 0.3, 3.0),
        "trial_vectors": draw_trial_vectors(jax.random.fold_in(streams_of[3], 71), 0),
    }


epsilon = 1e-06

def reference(integrals, energy_gaps, trial_vectors):
    trial_half = trial_vectors.astype(jnp.bfloat16)
    aux_totals = lax.dot_general(integrals, trial_half, (((0,), (0,)), ((), ())), preferred_element_type=jnp.float32)
    aux_half = aux_totals.astype(jnp.bfloat16)
    coupled = jnp.dot(integrals, aux_half, preferred_element_type=jnp.float32)
    sigma_vectors = energy_gaps[:, None] * trial_vectors + 2.0 * coupled
    subspace = lax.dot_general(trial_vectors, sigma_vectors, (((0,), (0,)), ((), ())), precision=lax.Precision.HIGHEST, preferred_element_type=jnp.float32) / PAIRS
    intersection = lax.optimization_barrier(jnp.sum(trial_vectors * trial_vectors, axis=0)) / PAIRS
    rayleigh = jnp.diagonal(subspace) / (intersection + epsilon)
    residuals = sigma_vectors - trial_vectors * rayleigh[None, :]
    residual_norms = jnp.sqrt(lax.optimization_barrier(jnp.sum(residuals * residuals, axis=0)) / PAIRS + epsilon)
    return (sigma_vectors, subspace, residuals, residual_norms)
```

```python
import jax
import jax.numpy as jnp
from jax import lax
from jax.experimental import pallas as pl
from jax.experimental.pallas import tpu as pltpu
from jax.sharding import Mesh
from jax.sharding import PartitionSpec as P

PAIR = ("z", "x")
AUX = ("y", "c")
ALL = ("z", "x", "y", "c")

epsilon = 1e-06
BF = jnp.bfloat16
F32 = jnp.float32
NT = (((1,), (1,)), ((), ()))
VMEM = pl.BlockSpec(memory_space=pltpu.VMEM)
HBM = pl.BlockSpec(memory_space=pltpu.HBM)
CHUNKS = 12
FLIGHT = 6
TOTALS_LIMIT = 60 * 1024 * 1024
COUPLED_LIMIT = 46 << 20


def split_two(value):
    high = value.astype(BF).astype(F32)
    return high, (value - high).astype(BF).astype(F32)


def totals_kernel(groups, integrals, trial, gaps, out, held, x_ref, gap_ref, stats, sems, small):
    pairs, aux = integrals.shape
    rows = pairs // CHUNKS

    def copy(n):
        return pltpu.make_async_copy(integrals.at[pl.ds(n * rows, rows)], held.at[pl.ds(n * rows, rows)], sems.at[n])

    x_copy = pltpu.make_async_copy(trial, x_ref, small.at[0])
    gap_copy = pltpu.make_async_copy(gaps, gap_ref, small.at[1])
    x_copy.start()
    gap_copy.start()
    for n in range(FLIGHT):
        copy(n).start()
    x_copy.wait()
    gap_copy.wait()
    x = x_ref[...]
    gx = x * gap_ref[...]
    x_high, x_low = split_two(x)
    g_high, g_low = split_two(gx)
    half = x_high.astype(BF)
    low = x_low.astype(BF)
    left = jnp.concatenate([half, low], axis=0)
    right = jnp.concatenate([g_high.astype(BF), g_low.astype(BF)], axis=0)
    both = lax.dot_general(left, right, NT, preferred_element_type=F32)
    vecs = x.shape[0]
    gram = both[:vecs, :vecs] + both[:vecs, vecs:] + both[vecs:, :vecs]
    squares = jnp.sum(x * x, axis=1, keepdims=True)
    wide = jnp.concatenate([gram, jnp.broadcast_to(squares, (vecs, vecs))], axis=1)
    high, low_part = split_two(wide)
    per = vecs // groups
    stats[...] = jnp.zeros_like(stats)
    for j in range(groups):
        stats[j, 0:per, :] = high[j * per : (j + 1) * per]
        stats[j, per : 2 * per, :] = low_part[j * per : (j + 1) * per]
    total = None
    for n in range(CHUNKS):
        copy(n).wait()
        if n + FLIGHT < CHUNKS:
            copy(n + FLIGHT).start()
        block = held[n * rows : (n + 1) * rows, :]
        part = jnp.dot(half[:, n * rows : (n + 1) * rows], block, preferred_element_type=F32)
        total = part if total is None else total + part
    columns = aux // 128
    tiles = (vecs // 8) * columns
    each = tiles // groups
    for t in range(tiles):
        r, q = divmod(t, columns)
        j, i = divmod(t, each)
        out[j, 8 * i : 8 * i + 8, :] = total[8 * r : 8 * r + 8, 128 * q : 128 * q + 128].astype(BF)
    out[:, 8 * each : 8 * each + 8, :] = stats[...].astype(BF)


def totals(integrals, trial, gaps, groups):
    pairs, aux = integrals.shape
    vecs = trial.shape[0]
    tall = (vecs // 8) * (aux // 128) // groups * 8 + 8
    return pl.pallas_call(
        lambda *refs: totals_kernel(groups, *refs),
        out_shape=jax.ShapeDtypeStruct((groups, tall, 128), BF),
        in_specs=[HBM, HBM, HBM],
        out_specs=VMEM,
        scratch_shapes=[
            pltpu.VMEM((pairs, aux), BF),
            pltpu.VMEM((vecs, pairs), F32),
            pltpu.VMEM((1, pairs), F32),
            pltpu.VMEM((groups, 8, 128), F32),
            pltpu.SemaphoreType.DMA((CHUNKS,)),
            pltpu.SemaphoreType.DMA((2,)),
        ],
        compiler_params=pltpu.CompilerParams(vmem_limit_bytes=TOTALS_LIMIT),
        cost_estimate=pl.CostEstimate(flops=2 * pairs * aux * 256, bytes_accessed=2 * pairs * aux, transcendentals=0),
        name="totals",
    )(integrals, trial, gaps)


def share(parts, per):
    total = jnp.sum(parts.astype(F32), axis=0)
    base = total.shape[0] - 8
    stat = total[base : base + per] + total[base + per : base + 2 * per]
    high = lax.reduce_precision(stat, 8, 7)
    tail = jnp.concatenate([high, stat - high, jnp.zeros((8 - 2 * per, 128), F32)], axis=0)
    mine = jnp.concatenate([total[:base], tail], axis=0).astype(BF)
    return jnp.broadcast_to(mine[None], parts.shape)


def aux_rows(gathered, rows):
    vecs, aux = rows.shape
    groups = gathered.shape[0]
    columns = aux // 128
    tiles = (vecs // 8) * columns
    each = tiles // groups
    for t in range(tiles):
        r, q = divmod(t, columns)
        j, i = divmod(t, each)
        rows[8 * r : 8 * r + 8, 128 * q : 128 * q + 128] = gathered[j, 8 * i : 8 * i + 8, :]


def coupled_kernel(integrals, kept, gathered, other, own, rows, held, sems):
    ys, cs = lax.axis_size("y"), lax.axis_size("c")
    block_rows = integrals.shape[0] // ys
    share_rows = block_rows // cs
    y, c = lax.axis_index("y"), lax.axis_index("c")
    copies = []
    for n in range(1, ys):
        copies.append(pltpu.make_async_copy(integrals.at[pl.ds(n * block_rows, block_rows)], held.at[n - 1], sems.at[n - 1]))
        copies[-1].start()
    aux_rows(gathered, rows)
    a = rows[...]
    gram = lax.dot_general(a, a, NT, preferred_element_type=F32)
    high, low = split_two(jnp.concatenate([gram, gram], axis=1))
    none = jnp.zeros((a.shape[0], share_rows), F32)
    own[ys] = jnp.concatenate([none, low], axis=1)
    other[ys] = jnp.concatenate([none, low], axis=1).astype(BF)
    for n in range(ys):
        if n:
            copies[n - 1].wait()
        source = held[n - 1] if n else kept[...]
        block = lax.dot_general(a, source, NT, preferred_element_type=F32)
        left, right = block[:, :share_rows], block[:, share_rows:]
        to = lax.rem(n + ys - y, ys)
        own[to] = jnp.concatenate([jnp.where(c == 0, left, right), high], axis=1)
        other[to] = jnp.concatenate([jnp.where(c == 0, right, left), high], axis=1).astype(BF)


def coupled(integrals, kept, gathered, vecs):
    pairs, aux = integrals.shape
    ys = lax.axis_size("y")
    block_rows = pairs // ys
    wide = block_rows // lax.axis_size("c") + 2 * vecs
    return pl.pallas_call(
        coupled_kernel,
        out_shape=[
            jax.ShapeDtypeStruct((ys + 1, vecs, wide), BF),
            jax.ShapeDtypeStruct((ys + 1, vecs, wide), F32),
        ],
        in_specs=[HBM, VMEM, VMEM],
        out_specs=[VMEM, VMEM],
        scratch_shapes=[
            pltpu.VMEM((vecs, aux), BF),
            pltpu.VMEM((ys - 1, block_rows, aux), BF),
            pltpu.SemaphoreType.DMA((ys - 1,)),
        ],
        compiler_params=pltpu.CompilerParams(vmem_limit_bytes=COUPLED_LIMIT),
        cost_estimate=pl.CostEstimate(flops=2 * pairs * aux * 256, bytes_accessed=2 * pairs * aux, transcendentals=0),
        name="coupled",
    )(integrals, kept, gathered)


def deal(own, other, vecs):
    ys, wide = own.shape[0] - 1, own.shape[2]
    total = own + other.astype(F32)
    total = total[:ys] + total[ys:]
    lane = lax.broadcasted_iota(jnp.int32, total.shape, 2)
    high = lax.reduce_precision(total, 8, 7)
    low = lax.reduce_precision(total - high, 8, 7)
    parts = jnp.where(lane < wide - vecs, high, low)
    mine = jnp.where(lane[0] < wide - 2 * vecs, total[0], parts[0])
    return mine, *[parts[k].astype(BF) for k in range(1, ys)]


def sigma_kernel(total_pairs, per, gathered, trial, gaps, kept, one, two, three, sigma, subspace, residuals, norms, grams):
    ys = 4
    y = lax.axis_index("y")
    vecs, rows = trial.shape
    block = kept[:, :rows]
    for part in (one, two, three):
        block = block + part[:, :rows].astype(F32)
    for k, part in enumerate((kept, one, two, three)):
        grams[lax.rem(y + ys - k, ys)] = part[:, rows:].astype(F32)
    gram = grams[0] + grams[1] + grams[2] + grams[3]
    gram = gram[:, :vecs] + gram[:, vecs:]
    groups, tall, _ = gathered.shape
    base = tall - 8
    wide = jnp.concatenate(
        [gathered[j, base : base + per, :].astype(F32) + gathered[j, base + per : base + 2 * per, :].astype(F32) for j in range(groups)],
        axis=0,
    )
    products = (wide[:, :vecs] + 2.0 * gram) / total_pairs
    subspace[...] = products
    r = lax.broadcasted_iota(jnp.int32, (vecs, vecs), 0)
    q = lax.broadcasted_iota(jnp.int32, (vecs, vecs), 1)
    diagonal = jnp.sum(jnp.where(r == q, products, 0.0), axis=1, keepdims=True)
    rayleigh = diagonal / (wide[:, vecs : vecs + 1] / total_pairs + epsilon)
    x = trial[...]
    s = gaps[...] * x + 2.0 * block
    sigma[...] = s
    rest = s - rayleigh * x
    residuals[...] = rest
    sums = jnp.sum(rest * rest, axis=1, keepdims=True)
    line = jnp.sum(jnp.where(r == q, jnp.broadcast_to(sums, (vecs, vecs)), 0.0), axis=0, keepdims=True)
    norms[...] = jnp.concatenate([line, jnp.zeros_like(line)], axis=1)


def sigma_rows(total_pairs, per, gathered, trial, gaps, parts):
    vecs, rows = trial.shape
    return pl.pallas_call(
        lambda *refs: sigma_kernel(total_pairs, per, *refs),
        out_shape=[
            jax.ShapeDtypeStruct((vecs, rows), F32),
            jax.ShapeDtypeStruct((vecs, vecs), F32),
            jax.ShapeDtypeStruct((vecs, rows), F32),
            jax.ShapeDtypeStruct((1, 128), F32),
        ],
        in_specs=[VMEM] * 7,
        out_specs=[VMEM] * 4,
        scratch_shapes=[pltpu.VMEM((4, vecs, 128), F32)],
        compiler_params=pltpu.CompilerParams(vmem_limit_bytes=16 << 20),
        cost_estimate=pl.CostEstimate(flops=20 * trial.size, bytes_accessed=16 * trial.size, transcendentals=0),
        name="sigma_rows",
    )(gathered, trial, gaps, *parts)


def exchange(value, axis):
    return lax.all_to_all(value, axis, 0, 0, tiled=True)


def shifted(value, axis, by):
    n = lax.axis_size(axis)
    return lax.ppermute(value, axis, [(i, (i + by) % n) for i in range(n)])


def local(integrals, energy_gaps, trial_vectors):
    pairs, vecs = trial_vectors.shape
    groups = lax.axis_size(PAIR)
    ys, cs = lax.axis_size("y"), lax.axis_size("c")
    total_pairs = float(pairs * groups)
    per = vecs // groups
    share_rows = pairs // (ys * cs)
    trial = trial_vectors.T
    gaps = energy_gaps.reshape(1, pairs)
    parts = totals(integrals, trial, gaps, groups)
    mine = share(exchange(parts, PAIR), per)
    gathered = exchange(mine, PAIR)
    other, own = coupled(integrals, lax.slice_in_dim(integrals, 0, pairs // ys, axis=0), gathered, vecs)
    arrived = shifted(other, "c", 1)
    mine, *sent = deal(own, arrived, vecs)
    came = [shifted(block, "y", k + 1) for k, block in enumerate(sent)]
    first = (lax.axis_index("y") * cs + lax.axis_index("c")) * share_rows
    own_trial = lax.dynamic_slice_in_dim(trial, first, share_rows, 1)
    own_gaps = lax.dynamic_slice_in_dim(gaps, first, share_rows, 1)
    sigma, subspace, residuals, norms = sigma_rows(total_pairs, per, gathered, own_trial, own_gaps, [mine, *came])
    norms = norms + shifted(norms, "c", 1)
    everyone = ("z", "x", "y")
    copies = jnp.broadcast_to(norms, (lax.axis_size(everyone), 1, 128))
    sums = jnp.sum(exchange(copies, everyone), axis=(0, 1))[:vecs]
    residual_norms = jnp.sqrt(sums / total_pairs + epsilon)
    return (sigma.T, subspace, residuals.T, residual_norms)


def solution(mesh):
    finer = Mesh(mesh.devices.reshape(8, 4, 4, 2), ALL)
    return jax.shard_map(
        local,
        mesh=finer,
        in_specs=(P(PAIR, AUX), P(PAIR), P(PAIR, None)),
        out_specs=(P(ALL, None), P(), P(ALL, None), P()),
        check_vma=False,
    )
```

```python
import jax
import jax.numpy as jnp
from jax import lax
from jax.experimental import pallas as pl
from jax.experimental.pallas import tpu as pltpu
from jax.sharding import Mesh
from jax.sharding import PartitionSpec as P

PAIR = ("z", "x")
AUX = ("y", "c")
ALL = ("z", "x", "y", "c")

epsilon = 1e-06
BF = jnp.bfloat16
F32 = jnp.float32
NT = (((1,), (1,)), ((), ()))
VMEM = pl.BlockSpec(memory_space=pltpu.VMEM)
HBM = pl.BlockSpec(memory_space=pltpu.HBM)
CHUNKS = 12
FLIGHT = 6
TOTALS_LIMIT = 60 * 1024 * 1024
COUPLED_LIMIT = 46 << 20


def split_two(value):
    high = value.astype(BF).astype(F32)
    return high, (value - high).astype(BF).astype(F32)


def totals_kernel(groups, integrals, trial, gaps, out, held, x_ref, gap_ref, stats, sems, small):
    pairs, aux = integrals.shape
    rows = pairs // CHUNKS

    def copy(n):
        return pltpu.make_async_copy(integrals.at[pl.ds(n * rows, rows)], held.at[pl.ds(n * rows, rows)], sems.at[n])

    x_copy = pltpu.make_async_copy(trial, x_ref, small.at[0])
    gap_copy = pltpu.make_async_copy(gaps, gap_ref, small.at[1])
    x_copy.start()
    gap_copy.start()
    for n in range(FLIGHT):
        copy(n).start()
    x_copy.wait()
    gap_copy.wait()
    x = x_ref[...]
    gx = x * gap_ref[...]
    x_high, x_low = split_two(x)
    g_high, g_low = split_two(gx)
    half = x_high.astype(BF)
    low = x_low.astype(BF)
    left = jnp.concatenate([half, low], axis=0)
    right = jnp.concatenate([g_high.astype(BF), g_low.astype(BF)], axis=0)
    both = lax.dot_general(left, right, NT, preferred_element_type=F32)
    vecs = x.shape[0]
    gram = both[:vecs, :vecs] + both[:vecs, vecs:] + both[vecs:, :vecs]
    squares = jnp.sum(x * x, axis=1, keepdims=True)
    wide = jnp.concatenate([gram, jnp.broadcast_to(squares, (vecs, vecs))], axis=1)
    high, low_part = split_two(wide)
    per = vecs // groups
    stats[...] = jnp.zeros_like(stats)
    for j in range(groups):
        stats[j, 0:per, :] = high[j * per : (j + 1) * per]
        stats[j, per : 2 * per, :] = low_part[j * per : (j + 1) * per]
    total = None
    for n in range(CHUNKS):
        copy(n).wait()
        if n + FLIGHT < CHUNKS:
            copy(n + FLIGHT).start()
        block = held[n * rows : (n + 1) * rows, :]
        part = jnp.dot(half[:, n * rows : (n + 1) * rows], block, preferred_element_type=F32)
        total = part if total is None else total + part
    columns = aux // 128
    tiles = (vecs // 8) * columns
    each = tiles // groups
    for t in range(tiles):
        r, q = divmod(t, columns)
        j, i = divmod(t, each)
        out[j, 8 * i : 8 * i + 8, :] = total[8 * r : 8 * r + 8, 128 * q : 128 * q + 128].astype(BF)
    out[:, 8 * each : 8 * each + 8, :] = stats[...].astype(BF)


def totals(integrals, trial, gaps, groups):
    pairs, aux = integrals.shape
    vecs = trial.shape[0]
    tall = (vecs // 8) * (aux // 128) // groups * 8 + 8
    return pl.pallas_call(
        lambda *refs: totals_kernel(groups, *refs),
        out_shape=jax.ShapeDtypeStruct((groups, tall, 128), BF),
        in_specs=[HBM, HBM, HBM],
        out_specs=VMEM,
        scratch_shapes=[
            pltpu.VMEM((pairs, aux), BF),
            pltpu.VMEM((vecs, pairs), F32),
            pltpu.VMEM((1, pairs), F32),
            pltpu.VMEM((groups, 8, 128), F32),
            pltpu.SemaphoreType.DMA((CHUNKS,)),
            pltpu.SemaphoreType.DMA((2,)),
        ],
        compiler_params=pltpu.CompilerParams(vmem_limit_bytes=TOTALS_LIMIT),
        cost_estimate=pl.CostEstimate(flops=2 * pairs * aux * 256, bytes_accessed=2 * pairs * aux, transcendentals=0),
        name="totals",
    )(integrals, trial, gaps)


def share(parts, per):
    total = jnp.sum(parts.astype(F32), axis=0)
    base = total.shape[0] - 8
    stat = total[base : base + per] + total[base + per : base + 2 * per]
    high = lax.reduce_precision(stat, 8, 7)
    tail = jnp.concatenate([high, stat - high, jnp.zeros((8 - 2 * per, 128), F32)], axis=0)
    mine = jnp.concatenate([total[:base], tail], axis=0).astype(BF)
    return jnp.broadcast_to(mine[None], parts.shape)


def aux_rows(gathered, rows):
    vecs, aux = rows.shape
    groups = gathered.shape[0]
    columns = aux // 128
    tiles = (vecs // 8) * columns
    each = tiles // groups
    for t in range(tiles):
        r, q = divmod(t, columns)
        j, i = divmod(t, each)
        rows[8 * r : 8 * r + 8, 128 * q : 128 * q + 128] = gathered[j, 8 * i : 8 * i + 8, :]


def coupled_kernel(integrals, kept, gathered, other, own, rows, held, sems):
    ys, cs = lax.axis_size("y"), lax.axis_size("c")
    saved = kept.shape[0]
    share_rows = integrals.shape[0] // (ys * cs)
    y, c = lax.axis_index("y"), lax.axis_index("c")
    size = held.shape[1]
    copies = [
        pltpu.make_async_copy(integrals.at[pl.ds(saved + n * size, size)], held.at[n], sems.at[n])
        for n in range(held.shape[0])
    ]
    for copy in copies:
        copy.start()
    aux_rows(gathered, rows)
    a = rows[...]
    gram = lax.dot_general(a, a, NT, preferred_element_type=F32)
    high, low = split_two(jnp.concatenate([gram, gram], axis=1))
    none = jnp.zeros((a.shape[0], share_rows), F32)
    low = jnp.concatenate([none, low], axis=1)
    own[ys] = low
    other[ys] = low.astype(BF)
    for n in range(ys):
        own[n, :, share_rows:] = high
        other[n, :, share_rows:] = high.astype(BF)

    def emit(first, source):
        block = lax.dot_general(a, source, NT, preferred_element_type=F32)
        for u in range(source.shape[0] // share_rows):
            n, half = divmod(first // share_rows + u, cs)
            to = lax.rem(n + ys - y, ys)
            piece = block[:, u * share_rows : (u + 1) * share_rows]

            @pl.when(c == half)
            def _():
                own[to, :, :share_rows] = piece

            @pl.when(c != half)
            def _():
                other[to, :, :share_rows] = piece.astype(BF)

    emit(0, kept[...])
    for n, copy in enumerate(copies):
        copy.wait()
        emit(saved + n * size, held[n])


def coupled(integrals, kept, gathered, vecs):
    pairs, aux = integrals.shape
    ys = lax.axis_size("y")
    wide = pairs // (ys * lax.axis_size("c")) + 2 * vecs
    waits = 2
    return pl.pallas_call(
        coupled_kernel,
        out_shape=[
            jax.ShapeDtypeStruct((ys + 1, vecs, wide), BF),
            jax.ShapeDtypeStruct((ys + 1, vecs, wide), F32),
        ],
        in_specs=[HBM, VMEM, VMEM],
        out_specs=[VMEM, VMEM],
        scratch_shapes=[
            pltpu.VMEM((vecs, aux), BF),
            pltpu.VMEM((waits, (pairs - kept.shape[0]) // waits, aux), BF),
            pltpu.SemaphoreType.DMA((waits,)),
        ],
        compiler_params=pltpu.CompilerParams(vmem_limit_bytes=COUPLED_LIMIT),
        cost_estimate=pl.CostEstimate(flops=2 * pairs * aux * 256, bytes_accessed=2 * pairs * aux, transcendentals=0),
        name="coupled",
    )(integrals, kept, gathered)


def deal(own, other, vecs):
    ys, wide = own.shape[0] - 1, own.shape[2]
    total = own + other.astype(F32)
    total = total[:ys] + total[ys:]
    lane = lax.broadcasted_iota(jnp.int32, total.shape, 2)
    high = lax.reduce_precision(total, 8, 7)
    low = lax.reduce_precision(total - high, 8, 7)
    parts = jnp.where(lane < wide - vecs, high, low)
    mine = jnp.where(lane[0] < wide - 2 * vecs, total[0], parts[0])
    return mine, *[parts[k].astype(BF) for k in range(1, ys)]


def sigma_kernel(total_pairs, per, gathered, trial, gaps, kept, one, two, three, sigma, subspace, residuals, norms, grams):
    ys = 4
    y = lax.axis_index("y")
    vecs, rows = trial.shape
    block = kept[:, :rows]
    for part in (one, two, three):
        block = block + part[:, :rows].astype(F32)
    for k, part in enumerate((kept, one, two, three)):
        grams[lax.rem(y + ys - k, ys)] = part[:, rows:].astype(F32)
    gram = grams[0] + grams[1] + grams[2] + grams[3]
    gram = gram[:, :vecs] + gram[:, vecs:]
    groups, tall, _ = gathered.shape
    base = tall - 8
    wide = jnp.concatenate(
        [gathered[j, base : base + per, :].astype(F32) + gathered[j, base + per : base + 2 * per, :].astype(F32) for j in range(groups)],
        axis=0,
    )
    products = (wide[:, :vecs] + 2.0 * gram) / total_pairs
    subspace[...] = products
    r = lax.broadcasted_iota(jnp.int32, (vecs, vecs), 0)
    q = lax.broadcasted_iota(jnp.int32, (vecs, vecs), 1)
    diagonal = jnp.sum(jnp.where(r == q, products, 0.0), axis=1, keepdims=True)
    rayleigh = diagonal / (wide[:, vecs : vecs + 1] / total_pairs + epsilon)
    x = trial[...]
    s = gaps[...] * x + 2.0 * block
    sigma[...] = s
    rest = s - rayleigh * x
    residuals[...] = rest
    sums = jnp.sum(rest * rest, axis=1, keepdims=True)
    line = jnp.sum(jnp.where(r == q, jnp.broadcast_to(sums, (vecs, vecs)), 0.0), axis=0, keepdims=True)
    norms[...] = jnp.concatenate([line, jnp.zeros_like(line)], axis=1)


def sigma_rows(total_pairs, per, gathered, trial, gaps, parts):
    vecs, rows = trial.shape
    return pl.pallas_call(
        lambda *refs: sigma_kernel(total_pairs, per, *refs),
        out_shape=[
            jax.ShapeDtypeStruct((vecs, rows), F32),
            jax.ShapeDtypeStruct((vecs, vecs), F32),
            jax.ShapeDtypeStruct((vecs, rows), F32),
            jax.ShapeDtypeStruct((1, 128), F32),
        ],
        in_specs=[VMEM] * 7,
        out_specs=[VMEM] * 4,
        scratch_shapes=[pltpu.VMEM((4, vecs, 128), F32)],
        compiler_params=pltpu.CompilerParams(vmem_limit_bytes=16 << 20),
        cost_estimate=pl.CostEstimate(flops=20 * trial.size, bytes_accessed=16 * trial.size, transcendentals=0),
        name="sigma_rows",
    )(gathered, trial, gaps, *parts)


def exchange(value, axis):
    return lax.all_to_all(value, axis, 0, 0, tiled=True)


def shifted(value, axis, by):
    n = lax.axis_size(axis)
    return lax.ppermute(value, axis, [(i, (i + by) % n) for i in range(n)])


def local(integrals, energy_gaps, trial_vectors):
    pairs, vecs = trial_vectors.shape
    groups = lax.axis_size(PAIR)
    ys, cs = lax.axis_size("y"), lax.axis_size("c")
    total_pairs = float(pairs * groups)
    per = vecs // groups
    share_rows = pairs // (ys * cs)
    trial = trial_vectors.T
    gaps = energy_gaps.reshape(1, pairs)
    parts = totals(integrals, trial, gaps, groups)
    mine = share(exchange(parts, PAIR), per)
    first = (lax.axis_index("y") * cs + lax.axis_index("c")) * share_rows
    own_trial = lax.dynamic_slice_in_dim(trial, first, share_rows, 1)
    own_gaps = lax.dynamic_slice_in_dim(gaps, first, share_rows, 1)
    kept = lax.slice_in_dim(integrals, 0, pairs // ys, axis=0)
    mine, own_trial, own_gaps, kept = lax.optimization_barrier((mine, own_trial, own_gaps, kept))
    gathered = exchange(mine, PAIR)
    other, own = coupled(integrals, kept, gathered, vecs)
    arrived = shifted(other, "c", 1)
    mine, *sent = deal(own, arrived, vecs)
    far = shifted(sent[1], "y", 2)
    came = [shifted(sent[0], "y", 1), far, shifted(sent[2], "y", 3)]
    sigma, subspace, residuals, norms = sigma_rows(total_pairs, per, gathered, own_trial, own_gaps, [mine, *came])
    norms = norms + shifted(norms, "c", 1)
    everyone = ("z", "x", "y")
    copies = jnp.broadcast_to(norms, (lax.axis_size(everyone), 1, 128))
    sums = jnp.sum(exchange(copies, everyone), axis=(0, 1))[:vecs]
    residual_norms = jnp.sqrt(sums / total_pairs + epsilon)
    return (sigma.T, subspace, residuals.T, residual_norms)


def solution(mesh):
    finer = Mesh(mesh.devices.reshape(8, 4, 4, 2), ALL)
    return jax.shard_map(
        local,
        mesh=finer,
        in_specs=(P(PAIR, AUX), P(PAIR), P(PAIR, None)),
        out_specs=(P(ALL, None), P(), P(ALL, None), P()),
        check_vma=False,
    )
```

```python
import jax
import jax.numpy as jnp
from jax import lax
from jax.experimental import pallas as pl
from jax.experimental.pallas import tpu as pltpu
from jax.sharding import Mesh
from jax.sharding import PartitionSpec as P

PAIR = ("z", "x")
AUX = ("y", "c")
ALL = ("z", "x", "y", "c")

epsilon = 1e-06
BF = jnp.bfloat16
F32 = jnp.float32
NT = (((1,), (1,)), ((), ()))
VMEM = pl.BlockSpec(memory_space=pltpu.VMEM)
HBM = pl.BlockSpec(memory_space=pltpu.HBM)
CHUNKS = 6
FIRST = 2
FLIGHT = 4
TOTALS_LIMIT = 60 * 1024 * 1024
COUPLED_LIMIT = 46 << 20


def split_two(value):
    high = value.astype(BF).astype(F32)
    return high, (value - high).astype(BF).astype(F32)


def totals_kernel(groups, integrals, trial, gaps, out, held, x_ref, gap_ref, stats, sems, small):
    pairs, aux = integrals.shape
    rows = pairs // CHUNKS

    def copy(n):
        return pltpu.make_async_copy(integrals.at[pl.ds(n * rows, rows)], held.at[pl.ds(n * rows, rows)], sems.at[n])

    x_copy = pltpu.make_async_copy(trial, x_ref, small.at[0])
    gap_copy = pltpu.make_async_copy(gaps, gap_ref, small.at[1])
    x_copy.start()
    gap_copy.start()
    for n in range(FIRST):
        copy(n).start()
    x_copy.wait()
    gap_copy.wait()
    for n in range(FIRST, FLIGHT):
        copy(n).start()
    vecs = trial.shape[0]
    total = both = squares = None
    for n in range(CHUNKS):
        x = x_ref[:, n * rows : (n + 1) * rows]
        x_high, x_low = split_two(x)
        g_high, g_low = split_two(x * gap_ref[:, n * rows : (n + 1) * rows])
        half = x_high.astype(BF)
        left = jnp.concatenate([half, x_low.astype(BF)], axis=0)
        right = jnp.concatenate([g_high.astype(BF), g_low.astype(BF)], axis=0)
        pieces = lax.dot_general(left, right, NT, preferred_element_type=F32)
        square = jnp.sum(x * x, axis=1, keepdims=True)
        copy(n).wait()
        if n + FLIGHT < CHUNKS:
            copy(n + FLIGHT).start()
        part = jnp.dot(half, held[n * rows : (n + 1) * rows, :], preferred_element_type=F32)
        total, both, squares = (part, pieces, square) if n == 0 else (total + part, both + pieces, squares + square)
    gram = both[:vecs, :vecs] + both[:vecs, vecs:] + both[vecs:, :vecs]
    wide = jnp.concatenate([gram, jnp.broadcast_to(squares, (vecs, vecs))], axis=1)
    high, low_part = split_two(wide)
    per = vecs // groups
    stats[...] = jnp.zeros_like(stats)
    for j in range(groups):
        stats[j, 0:per, :] = high[j * per : (j + 1) * per]
        stats[j, per : 2 * per, :] = low_part[j * per : (j + 1) * per]
    columns = aux // 128
    tiles = (vecs // 8) * columns
    each = tiles // groups
    for t in range(tiles):
        r, q = divmod(t, columns)
        j, i = divmod(t, each)
        out[j, 8 * i : 8 * i + 8, :] = total[8 * r : 8 * r + 8, 128 * q : 128 * q + 128].astype(BF)
    out[:, 8 * each : 8 * each + 8, :] = stats[...].astype(BF)


def totals(integrals, trial, gaps, groups):
    pairs, aux = integrals.shape
    vecs = trial.shape[0]
    tall = (vecs // 8) * (aux // 128) // groups * 8 + 8
    return pl.pallas_call(
        lambda *refs: totals_kernel(groups, *refs),
        out_shape=jax.ShapeDtypeStruct((groups, tall, 128), BF),
        in_specs=[HBM, HBM, HBM],
        out_specs=VMEM,
        scratch_shapes=[
            pltpu.VMEM((pairs, aux), BF),
            pltpu.VMEM((vecs, pairs), F32),
            pltpu.VMEM((1, pairs), F32),
            pltpu.VMEM((groups, 8, 128), F32),
            pltpu.SemaphoreType.DMA((CHUNKS,)),
            pltpu.SemaphoreType.DMA((2,)),
        ],
        compiler_params=pltpu.CompilerParams(vmem_limit_bytes=TOTALS_LIMIT),
        cost_estimate=pl.CostEstimate(flops=2 * pairs * aux * 256, bytes_accessed=2 * pairs * aux, transcendentals=0),
        name="totals",
    )(integrals, trial, gaps)


def share(parts, per):
    total = jnp.sum(parts.astype(F32), axis=0)
    base = total.shape[0] - 8
    stat = total[base : base + per] + total[base + per : base + 2 * per]
    high = lax.reduce_precision(stat, 8, 7)
    tail = jnp.concatenate([high, stat - high, jnp.zeros((8 - 2 * per, 128), F32)], axis=0)
    mine = jnp.concatenate([total[:base], tail], axis=0).astype(BF)
    return jnp.broadcast_to(mine[None], parts.shape)


def aux_rows(gathered, rows):
    vecs, aux = rows.shape
    groups = gathered.shape[0]
    columns = aux // 128
    tiles = (vecs // 8) * columns
    each = tiles // groups
    for t in range(tiles):
        r, q = divmod(t, columns)
        j, i = divmod(t, each)
        rows[8 * r : 8 * r + 8, 128 * q : 128 * q + 128] = gathered[j, 8 * i : 8 * i + 8, :]


def coupled_kernel(integrals, kept, gathered, other, own, rows, held, sems):
    ys, cs = lax.axis_size("y"), lax.axis_size("c")
    saved = kept.shape[0]
    share_rows = integrals.shape[0] // (ys * cs)
    y, c = lax.axis_index("y"), lax.axis_index("c")
    size = held.shape[1]
    copies = [
        pltpu.make_async_copy(integrals.at[pl.ds(saved + n * size, size)], held.at[n], sems.at[n])
        for n in range(held.shape[0])
    ]
    for copy in copies:
        copy.start()
    aux_rows(gathered, rows)
    a = rows[...]
    vecs = a.shape[0]
    gram = lax.dot_general(a, a, NT, preferred_element_type=F32)
    half = vecs // 2
    corner = jnp.concatenate([gram[:half], gram[half:, half:]], axis=1)
    strip = jnp.concatenate([corner[8 * i : 8 * i + 8] for i in range(half // 8)], axis=1).astype(BF)
    for n in range(ys):
        own[n, vecs:, :] = strip.astype(F32)
        other[n, vecs:, :] = strip

    def emit(first, source):
        block = lax.dot_general(a, source, NT, preferred_element_type=F32)
        for u in range(source.shape[0] // share_rows):
            n, half = divmod(first // share_rows + u, cs)
            to = lax.rem(n + ys - y, ys)
            piece = block[:, u * share_rows : (u + 1) * share_rows]

            @pl.when(c == half)
            def _():
                own[to, :vecs, :] = piece

            @pl.when(c != half)
            def _():
                other[to, :vecs, :] = piece.astype(BF)

    emit(0, kept[...])
    for n, copy in enumerate(copies):
        copy.wait()
        emit(saved + n * size, held[n])


def coupled(integrals, kept, gathered, vecs):
    pairs, aux = integrals.shape
    ys = lax.axis_size("y")
    shape = (ys, vecs + 8, pairs // (ys * lax.axis_size("c")))
    waits = 2
    return pl.pallas_call(
        coupled_kernel,
        out_shape=[
            jax.ShapeDtypeStruct(shape, BF),
            jax.ShapeDtypeStruct(shape, F32),
        ],
        in_specs=[HBM, VMEM, VMEM],
        out_specs=[VMEM, VMEM],
        scratch_shapes=[
            pltpu.VMEM((vecs, aux), BF),
            pltpu.VMEM((waits, (pairs - kept.shape[0]) // waits, aux), BF),
            pltpu.SemaphoreType.DMA((waits,)),
        ],
        compiler_params=pltpu.CompilerParams(vmem_limit_bytes=COUPLED_LIMIT),
        cost_estimate=pl.CostEstimate(flops=2 * pairs * aux * 256, bytes_accessed=2 * pairs * aux, transcendentals=0),
        name="coupled",
    )(integrals, kept, gathered)


def deal(own, other):
    total = own + other.astype(F32)
    return total[0], *[total[k].astype(BF) for k in range(1, own.shape[0])]


def sigma_kernel(total_pairs, per, gathered, trial, gaps, kept, one, two, three, sigma, subspace, residuals, norms, grams):
    ys = 4
    y = lax.axis_index("y")
    vecs, rows = trial.shape
    block = kept[:vecs, :]
    for part in (one, two, three):
        block = block + part[:vecs, :].astype(F32)
    for k, part in enumerate((kept, one, two, three)):
        grams[lax.rem(y + ys - k, ys)] = part[vecs:, :].astype(BF).astype(F32)
    strip = grams[0] + grams[1] + grams[2] + grams[3]
    half = vecs // 2
    lanes = half + vecs
    corner = jnp.concatenate([strip[:, lanes * i : lanes * i + lanes] for i in range(half // 8)], axis=0)
    turned = jnp.transpose(jnp.concatenate([corner, jnp.zeros((half, 128 - lanes), F32)], axis=1))
    lower = jnp.concatenate([turned[half:vecs], corner[:, vecs:]], axis=1)
    gram = jnp.concatenate([corner[:, :vecs], lower], axis=0)
    groups, tall, _ = gathered.shape
    base = tall - 8
    wide = jnp.concatenate(
        [gathered[j, base : base + per, :].astype(F32) + gathered[j, base + per : base + 2 * per, :].astype(F32) for j in range(groups)],
        axis=0,
    )
    products = (wide[:, :vecs] + 2.0 * gram) / total_pairs
    subspace[...] = products
    r = lax.broadcasted_iota(jnp.int32, (vecs, vecs), 0)
    q = lax.broadcasted_iota(jnp.int32, (vecs, vecs), 1)
    diagonal = jnp.sum(jnp.where(r == q, products, 0.0), axis=1, keepdims=True)
    rayleigh = diagonal / (wide[:, vecs : vecs + 1] / total_pairs + epsilon)
    x = trial[...]
    s = gaps[...] * x + 2.0 * block
    sigma[...] = s
    rest = s - rayleigh * x
    residuals[...] = rest
    sums = jnp.sum(rest * rest, axis=1, keepdims=True)
    line = jnp.sum(jnp.where(r == q, jnp.broadcast_to(sums, (vecs, vecs)), 0.0), axis=0, keepdims=True)
    norms[...] = jnp.concatenate([line, jnp.zeros_like(line)], axis=1)


def sigma_rows(total_pairs, per, gathered, trial, gaps, parts):
    vecs, rows = trial.shape
    return pl.pallas_call(
        lambda *refs: sigma_kernel(total_pairs, per, *refs),
        out_shape=[
            jax.ShapeDtypeStruct((vecs, rows), F32),
            jax.ShapeDtypeStruct((vecs, vecs), F32),
            jax.ShapeDtypeStruct((vecs, rows), F32),
            jax.ShapeDtypeStruct((1, 128), F32),
        ],
        in_specs=[VMEM] * 7,
        out_specs=[VMEM] * 4,
        scratch_shapes=[pltpu.VMEM((4, 8, rows), F32)],
        compiler_params=pltpu.CompilerParams(vmem_limit_bytes=16 << 20),
        cost_estimate=pl.CostEstimate(flops=20 * trial.size, bytes_accessed=16 * trial.size, transcendentals=0),
        name="sigma_rows",
    )(gathered, trial, gaps, *parts)


def exchange(value, axis):
    return lax.all_to_all(value, axis, 0, 0, tiled=True)


def shifted(value, axis, by):
    n = lax.axis_size(axis)
    return lax.ppermute(value, axis, [(i, (i + by) % n) for i in range(n)])


def local(integrals, energy_gaps, trial_vectors):
    pairs, vecs = trial_vectors.shape
    groups = lax.axis_size(PAIR)
    ys, cs = lax.axis_size("y"), lax.axis_size("c")
    total_pairs = float(pairs * groups)
    per = vecs // groups
    share_rows = pairs // (ys * cs)
    trial = trial_vectors.T
    gaps = energy_gaps.reshape(1, pairs)
    parts = totals(integrals, trial, gaps, groups)
    mine = share(exchange(parts, PAIR), per)
    first = (lax.axis_index("y") * cs + lax.axis_index("c")) * share_rows
    own_trial = lax.dynamic_slice_in_dim(trial, first, share_rows, 1)
    own_gaps = lax.dynamic_slice_in_dim(gaps, first, share_rows, 1)
    kept = lax.slice_in_dim(integrals, 0, pairs // ys, axis=0)
    mine, own_trial, own_gaps, kept = lax.optimization_barrier((mine, own_trial, own_gaps, kept))
    gathered = exchange(mine, PAIR)
    other, own = coupled(integrals, kept, gathered, vecs)
    arrived = shifted(other, "c", 1)
    mine, *sent = deal(own, arrived)
    far = shifted(sent[1], "y", 2)
    came = [shifted(sent[0], "y", 1), far, shifted(sent[2], "y", 3)]
    sigma, subspace, residuals, norms = sigma_rows(total_pairs, per, gathered, own_trial, own_gaps, [mine, *came])
    norms = norms + shifted(norms, "c", 1)
    everyone = ("z", "x", "y")
    copies = jnp.broadcast_to(norms, (lax.axis_size(everyone), 1, 128))
    sums = jnp.sum(exchange(copies, everyone), axis=(0, 1))[:vecs]
    residual_norms = jnp.sqrt(sums / total_pairs + epsilon)
    return (sigma.T, subspace, residuals.T, residual_norms)


def solution(mesh):
    finer = Mesh(mesh.devices.reshape(8, 4, 4, 2), ALL)
    return jax.shard_map(
        local,
        mesh=finer,
        in_specs=(P(PAIR, AUX), P(PAIR), P(PAIR, None)),
        out_specs=(P(ALL, None), P(), P(ALL, None), P()),
        check_vma=False,
    )
```

```python
import jax
import jax.numpy as jnp
from jax import lax
from jax.experimental import pallas as pl
from jax.experimental.pallas import tpu as pltpu
from jax.sharding import Mesh
from jax.sharding import PartitionSpec as P

PAIR = ("z", "x")
AUX = ("y", "c")
ALL = ("z", "x", "y", "c")

epsilon = 1e-06
BF = jnp.bfloat16
F32 = jnp.float32
NT = (((1,), (1,)), ((), ()))
VMEM = pl.BlockSpec(memory_space=pltpu.VMEM)
HBM = pl.BlockSpec(memory_space=pltpu.HBM)
CHUNKS = 6
FIRST = 2
FLIGHT = 4
TOTALS_LIMIT = 60 * 1024 * 1024
COUPLED_LIMIT = 46 << 20


def split_two(value):
    high = value.astype(BF).astype(F32)
    return high, (value - high).astype(BF).astype(F32)


def totals_kernel(groups, integrals, trial, gaps, out, held, x_ref, gap_ref, stats, sems, small):
    pairs, aux = integrals.shape
    rows = pairs // CHUNKS

    def copy(n):
        return pltpu.make_async_copy(integrals.at[pl.ds(n * rows, rows)], held.at[pl.ds(n * rows, rows)], sems.at[n])

    x_copy = pltpu.make_async_copy(trial, x_ref, small.at[0])
    gap_copy = pltpu.make_async_copy(gaps, gap_ref, small.at[1])
    x_copy.start()
    gap_copy.start()
    for n in range(FIRST):
        copy(n).start()
    x_copy.wait()
    gap_copy.wait()
    for n in range(FIRST, FLIGHT):
        copy(n).start()
    vecs = trial.shape[0]
    total = both = squares = None
    for n in range(CHUNKS):
        x = x_ref[:, n * rows : (n + 1) * rows]
        x_high, x_low = split_two(x)
        g_high, g_low = split_two(x * gap_ref[:, n * rows : (n + 1) * rows])
        half = x_high.astype(BF)
        left = jnp.concatenate([half, x_low.astype(BF)], axis=0)
        right = jnp.concatenate([g_high.astype(BF), g_low.astype(BF)], axis=0)
        pieces = lax.dot_general(left, right, NT, preferred_element_type=F32)
        square = jnp.sum(x * x, axis=1, keepdims=True)
        copy(n).wait()
        if n + FLIGHT < CHUNKS:
            copy(n + FLIGHT).start()
        part = jnp.dot(half, held[n * rows : (n + 1) * rows, :], preferred_element_type=F32)
        total, both, squares = (part, pieces, square) if n == 0 else (total + part, both + pieces, squares + square)
    gram = both[:vecs, :vecs] + both[:vecs, vecs:] + both[vecs:, :vecs]
    wide = jnp.concatenate([gram, jnp.broadcast_to(squares, (vecs, vecs))], axis=1)
    high, low_part = split_two(wide)
    per = vecs // groups
    stats[...] = jnp.zeros_like(stats)
    for j in range(groups):
        stats[j, 0:per, :] = high[j * per : (j + 1) * per]
        stats[j, per : 2 * per, :] = low_part[j * per : (j + 1) * per]
    columns = aux // 128
    tiles = (vecs // 8) * columns
    each = tiles // groups
    for t in range(tiles):
        r, q = divmod(t, columns)
        j, i = divmod(t, each)
        out[j, 8 * i : 8 * i + 8, :] = total[8 * r : 8 * r + 8, 128 * q : 128 * q + 128].astype(BF)
    out[:, 8 * each : 8 * each + 8, :] = stats[...].astype(BF)


def totals(integrals, trial, gaps, groups):
    pairs, aux = integrals.shape
    vecs = trial.shape[0]
    tall = (vecs // 8) * (aux // 128) // groups * 8 + 8
    return pl.pallas_call(
        lambda *refs: totals_kernel(groups, *refs),
        out_shape=jax.ShapeDtypeStruct((groups, tall, 128), BF),
        in_specs=[HBM, HBM, HBM],
        out_specs=VMEM,
        scratch_shapes=[
            pltpu.VMEM((pairs, aux), BF),
            pltpu.VMEM((vecs, pairs), F32),
            pltpu.VMEM((1, pairs), F32),
            pltpu.VMEM((groups, 8, 128), F32),
            pltpu.SemaphoreType.DMA((CHUNKS,)),
            pltpu.SemaphoreType.DMA((2,)),
        ],
        compiler_params=pltpu.CompilerParams(vmem_limit_bytes=TOTALS_LIMIT),
        cost_estimate=pl.CostEstimate(flops=2 * pairs * aux * 256, bytes_accessed=2 * pairs * aux, transcendentals=0),
        name="totals",
    )(integrals, trial, gaps)


def share(parts, per):
    total = jnp.sum(parts.astype(F32), axis=0)
    base = total.shape[0] - 8
    stat = total[base : base + per] + total[base + per : base + 2 * per]
    high = lax.reduce_precision(stat, 8, 7)
    tail = jnp.concatenate([high, stat - high, jnp.zeros((8 - 2 * per, 128), F32)], axis=0)
    mine = jnp.concatenate([total[:base], tail], axis=0).astype(BF)
    return jnp.broadcast_to(mine[None], parts.shape)


def aux_rows(gathered, rows):
    vecs, aux = rows.shape
    groups = gathered.shape[0]
    columns = aux // 128
    tiles = (vecs // 8) * columns
    each = tiles // groups
    for t in range(tiles):
        r, q = divmod(t, columns)
        j, i = divmod(t, each)
        rows[8 * r : 8 * r + 8, 128 * q : 128 * q + 128] = gathered[j, 8 * i : 8 * i + 8, :]


def coupled_kernel(integrals, kept, gathered, other, own, rows, held, sems):
    ys, cs = lax.axis_size("y"), lax.axis_size("c")
    saved = kept.shape[0]
    share_rows = integrals.shape[0] // (ys * cs)
    y, c = lax.axis_index("y"), lax.axis_index("c")
    size = held.shape[1]
    copies = [
        pltpu.make_async_copy(integrals.at[pl.ds(saved + n * size, size)], held.at[n], sems.at[n])
        for n in range(held.shape[0])
    ]
    for copy in copies:
        copy.start()
    aux_rows(gathered, rows)
    a = rows[...]
    vecs = a.shape[0]
    gram = lax.dot_general(a, a, NT, preferred_element_type=F32)
    half = vecs // 2
    corner = jnp.concatenate([gram[:half], gram[half:, half:]], axis=1)
    strip = jnp.concatenate([corner[8 * i : 8 * i + 8] for i in range(half // 8)], axis=1).astype(BF)
    for n in range(ys):
        own[n, vecs:, :] = strip.astype(F32)
        other[n, vecs:, :] = strip

    def emit(first, source):
        block = lax.dot_general(a, source, NT, preferred_element_type=F32)
        for u in range(source.shape[0] // share_rows):
            n, half = divmod(first // share_rows + u, cs)
            to = lax.rem(n + ys - y, ys)
            piece = block[:, u * share_rows : (u + 1) * share_rows]

            @pl.when(c == half)
            def _():
                own[to, :vecs, :] = piece

            @pl.when(c != half)
            def _():
                other[to, :vecs, :] = piece.astype(BF)

    emit(0, kept[...])
    for n, copy in enumerate(copies):
        copy.wait()
        emit(saved + n * size, held[n])


def coupled(integrals, kept, gathered, vecs):
    pairs, aux = integrals.shape
    ys = lax.axis_size("y")
    shape = (ys, vecs + 8, pairs // (ys * lax.axis_size("c")))
    waits = 2
    return pl.pallas_call(
        coupled_kernel,
        out_shape=[
            jax.ShapeDtypeStruct(shape, BF),
            jax.ShapeDtypeStruct(shape, F32),
        ],
        in_specs=[HBM, VMEM, VMEM],
        out_specs=[VMEM, VMEM],
        scratch_shapes=[
            pltpu.VMEM((vecs, aux), BF),
            pltpu.VMEM((waits, (pairs - kept.shape[0]) // waits, aux), BF),
            pltpu.SemaphoreType.DMA((waits,)),
        ],
        compiler_params=pltpu.CompilerParams(vmem_limit_bytes=COUPLED_LIMIT),
        cost_estimate=pl.CostEstimate(flops=2 * pairs * aux * 256, bytes_accessed=2 * pairs * aux, transcendentals=0),
        name="coupled",
    )(integrals, kept, gathered)


def deal(own, other):
    total = own + other.astype(F32)
    return total[0], *[total[k].astype(BF) for k in range(1, own.shape[0])]


def sigma_kernel(total_pairs, stats, trial, gaps, kept, one, two, three, coupled_sum, rates, products, norms, grams):
    ys = 4
    y = lax.axis_index("y")
    vecs, rows = trial.shape
    for k, part in enumerate((kept, one, two, three)):
        grams[lax.rem(y + ys - k, ys)] = part[vecs:, :].astype(BF).astype(F32)
    strip = grams[0] + grams[1] + grams[2] + grams[3]
    half = vecs // 2
    lanes = half + vecs
    corner = jnp.concatenate([strip[:, lanes * i : lanes * i + lanes] for i in range(half // 8)], axis=0)
    turned = jnp.transpose(jnp.concatenate([corner, jnp.zeros((half, 128 - lanes), F32)], axis=1))
    lower = jnp.concatenate([turned[half:vecs], corner[:, vecs:]], axis=1)
    gram = jnp.concatenate([corner[:, :vecs], lower], axis=0)
    wide = stats[...]
    product = wide[:, :vecs] + 2.0 * gram
    products[...] = product
    r = lax.broadcasted_iota(jnp.int32, (vecs, vecs), 0)
    q = lax.broadcasted_iota(jnp.int32, (vecs, vecs), 1)
    diagonal = jnp.sum(jnp.where(r == q, product, 0.0), axis=1, keepdims=True)
    rayleigh = diagonal / total_pairs / (wide[:, vecs : vecs + 1] / total_pairs + epsilon)
    rates[...] = jnp.broadcast_to(rayleigh, rates.shape)
    block = kept[:vecs, :]
    for part in (one, two, three):
        block = block + part[:vecs, :].astype(F32)
    coupled_sum[...] = block
    x = trial[...]
    rest = gaps[...] * x + 2.0 * block - rayleigh * x
    sums = jnp.sum(rest * rest, axis=1, keepdims=True)
    line = jnp.sum(jnp.where(r == q, jnp.broadcast_to(sums, (vecs, vecs)), 0.0), axis=0, keepdims=True)
    norms[...] = jnp.concatenate([line, jnp.zeros_like(line)], axis=1)


def sigma_rows(total_pairs, stats, trial, gaps, parts):
    vecs, rows = trial.shape
    return pl.pallas_call(
        lambda *refs: sigma_kernel(total_pairs, *refs),
        out_shape=[
            jax.ShapeDtypeStruct((vecs, rows), F32),
            jax.ShapeDtypeStruct((vecs, 128), F32),
            jax.ShapeDtypeStruct((vecs, vecs), F32),
            jax.ShapeDtypeStruct((1, 128), F32),
        ],
        in_specs=[VMEM] * 7,
        out_specs=[VMEM] * 4,
        scratch_shapes=[pltpu.VMEM((4, 8, rows), F32)],
        compiler_params=pltpu.CompilerParams(vmem_limit_bytes=16 << 20),
        cost_estimate=pl.CostEstimate(flops=20 * trial.size, bytes_accessed=16 * trial.size, transcendentals=0),
        name="sigma_rows",
    )(stats, trial, gaps, *parts)


def finish_kernel(total_pairs, arrived, products, subspace, norms):
    subspace[...] = products[...] / total_pairs
    sums = jnp.sum(arrived[...], axis=0, keepdims=True)
    norms[...] = jnp.sqrt(sums / total_pairs + epsilon)[:, : norms.shape[1]]


def finish(total_pairs, arrived, products):
    return pl.pallas_call(
        lambda *refs: finish_kernel(total_pairs, *refs),
        out_shape=[jax.ShapeDtypeStruct(products.shape, F32), jax.ShapeDtypeStruct((1, products.shape[0]), F32)],
        in_specs=[VMEM] * 2,
        out_specs=[VMEM] * 2,
        compiler_params=pltpu.CompilerParams(vmem_limit_bytes=16 << 20),
        name="finish",
    )(arrived, products)


def exchange(value, axis):
    return lax.all_to_all(value, axis, 0, 0, tiled=True)


def shifted(value, axis, by):
    n = lax.axis_size(axis)
    return lax.ppermute(value, axis, [(i, (i + by) % n) for i in range(n)])


def local(integrals, energy_gaps, trial_vectors):
    pairs, vecs = trial_vectors.shape
    groups = lax.axis_size(PAIR)
    ys, cs = lax.axis_size("y"), lax.axis_size("c")
    total_pairs = float(pairs * groups)
    per = vecs // groups
    share_rows = pairs // (ys * cs)
    trial = trial_vectors.T
    gaps = energy_gaps.reshape(1, pairs)
    parts = totals(integrals, trial, gaps, groups)
    mine = share(exchange(parts, PAIR), per)
    first = (lax.axis_index("y") * cs + lax.axis_index("c")) * share_rows
    own_trial = lax.dynamic_slice_in_dim(trial, first, share_rows, 1)
    own_gaps = lax.dynamic_slice_in_dim(gaps, first, share_rows, 1)
    kept = lax.slice_in_dim(integrals, 0, pairs // ys, axis=0)
    mine, own_trial, own_gaps, kept = lax.optimization_barrier((mine, own_trial, own_gaps, kept))
    gathered = exchange(mine, PAIR)
    other, own = coupled(integrals, kept, gathered, vecs)
    arrived = shifted(other, "c", 1)
    mine, *sent = deal(own, arrived)
    far = shifted(sent[1], "y", 2)
    came = [shifted(sent[0], "y", 1), far, shifted(sent[2], "y", 3)]
    base = gathered.shape[1] - 8
    stats = gathered[:, base : base + per, :].astype(F32) + gathered[:, base + per : base + 2 * per, :].astype(F32)
    stats = stats.reshape(vecs, 128)
    coupled_sum, rates, products, norms = sigma_rows(total_pairs, stats, own_trial, own_gaps, [mine, *came])
    coupled_sum, own_trial, own_gaps = lax.optimization_barrier((coupled_sum, own_trial, own_gaps))
    sigma = own_gaps * own_trial + 2.0 * coupled_sum
    residuals = sigma - rates[:, :1] * own_trial
    norms = norms + shifted(norms, "c", 1)
    norms, sigma, residuals = lax.optimization_barrier((norms, sigma, residuals))
    everyone = ("z", "x", "y")
    copies = jnp.broadcast_to(norms, (lax.axis_size(everyone), 1, 128))
    arrived = exchange(copies, everyone).reshape(-1, 128)
    subspace, residual_norms = finish(total_pairs, arrived, products)
    residual_norms = residual_norms.reshape(vecs)
    return (sigma.T, subspace, residuals.T, residual_norms)


def solution(mesh):
    finer = Mesh(mesh.devices.reshape(8, 4, 4, 2), ALL)
    return jax.shard_map(
        local,
        mesh=finer,
        in_specs=(P(PAIR, AUX), P(PAIR), P(PAIR, None)),
        out_specs=(P(ALL, None), P(), P(ALL, None), P()),
        check_vma=False,
    )
```

```python
import jax
import jax.numpy as jnp
from jax import lax
from jax.experimental import pallas as pl
from jax.experimental.pallas import tpu as pltpu
from jax.sharding import Mesh
from jax.sharding import PartitionSpec as P

PAIR = ("z", "x")
AUX = ("y", "c")
ALL = ("z", "x", "y", "c")

epsilon = 1e-06
BF = jnp.bfloat16
F32 = jnp.float32
NT = (((1,), (1,)), ((), ()))
VMEM = pl.BlockSpec(memory_space=pltpu.VMEM)
HBM = pl.BlockSpec(memory_space=pltpu.HBM)
CHUNKS = 6
FIRST = 2
FLIGHT = 4
TOTALS_LIMIT = 60 * 1024 * 1024
COUPLED_LIMIT = 46 << 20


def split_two(value):
    high = value.astype(BF).astype(F32)
    return high, (value - high).astype(BF).astype(F32)


def totals_kernel(groups, integrals, trial, gaps, out, held, x_ref, gap_ref, stats, sems, small):
    pairs, aux = integrals.shape
    rows = pairs // CHUNKS

    def copy(n):
        return pltpu.make_async_copy(integrals.at[pl.ds(n * rows, rows)], held.at[pl.ds(n * rows, rows)], sems.at[n])

    x_copy = pltpu.make_async_copy(trial, x_ref, small.at[0])
    gap_copy = pltpu.make_async_copy(gaps, gap_ref, small.at[1])
    x_copy.start()
    gap_copy.start()
    for n in range(FIRST):
        copy(n).start()
    x_copy.wait()
    gap_copy.wait()
    for n in range(FIRST, FLIGHT):
        copy(n).start()
    vecs = trial.shape[0]
    total = both = squares = None
    for n in range(CHUNKS):
        x = x_ref[:, n * rows : (n + 1) * rows]
        x_high, x_low = split_two(x)
        g_high, g_low = split_two(x * gap_ref[:, n * rows : (n + 1) * rows])
        half = x_high.astype(BF)
        left = jnp.concatenate([half, x_low.astype(BF)], axis=0)
        right = jnp.concatenate([g_high.astype(BF), g_low.astype(BF)], axis=0)
        pieces = lax.dot_general(left, right, NT, preferred_element_type=F32)
        square = jnp.sum(x * x, axis=1, keepdims=True)
        copy(n).wait()
        if n + FLIGHT < CHUNKS:
            copy(n + FLIGHT).start()
        part = jnp.dot(half, held[n * rows : (n + 1) * rows, :], preferred_element_type=F32)
        total, both, squares = (part, pieces, square) if n == 0 else (total + part, both + pieces, squares + square)
    gram = both[:vecs, :vecs] + both[:vecs, vecs:] + both[vecs:, :vecs]
    wide = jnp.concatenate([gram, jnp.broadcast_to(squares, (vecs, vecs))], axis=1)
    high, low_part = split_two(wide)
    per = vecs // groups
    stats[...] = jnp.zeros_like(stats)
    for j in range(groups):
        stats[j, 0:per, :] = high[j * per : (j + 1) * per]
        stats[j, per : 2 * per, :] = low_part[j * per : (j + 1) * per]
    columns = aux // 128
    tiles = (vecs // 8) * columns
    each = tiles // groups
    for t in range(tiles):
        r, q = divmod(t, columns)
        j, i = divmod(t, each)
        out[j, 8 * i : 8 * i + 8, :] = total[8 * r : 8 * r + 8, 128 * q : 128 * q + 128].astype(BF)
    out[:, 8 * each : 8 * each + 8, :] = stats[...].astype(BF)


def totals(integrals, trial, gaps, groups):
    pairs, aux = integrals.shape
    vecs = trial.shape[0]
    tall = (vecs // 8) * (aux // 128) // groups * 8 + 8
    return pl.pallas_call(
        lambda *refs: totals_kernel(groups, *refs),
        out_shape=jax.ShapeDtypeStruct((groups, tall, 128), BF),
        in_specs=[HBM, HBM, HBM],
        out_specs=VMEM,
        scratch_shapes=[
            pltpu.VMEM((pairs, aux), BF),
            pltpu.VMEM((vecs, pairs), F32),
            pltpu.VMEM((1, pairs), F32),
            pltpu.VMEM((groups, 8, 128), F32),
            pltpu.SemaphoreType.DMA((CHUNKS,)),
            pltpu.SemaphoreType.DMA((2,)),
        ],
        compiler_params=pltpu.CompilerParams(vmem_limit_bytes=TOTALS_LIMIT),
        cost_estimate=pl.CostEstimate(flops=2 * pairs * aux * 256, bytes_accessed=2 * pairs * aux, transcendentals=0),
        name="totals",
    )(integrals, trial, gaps)


def share(parts, per):
    total = jnp.sum(parts.astype(F32), axis=0)
    base = total.shape[0] - 8
    stat = total[base : base + per] + total[base + per : base + 2 * per]
    high = lax.reduce_precision(stat, 8, 7)
    tail = jnp.concatenate([high, stat - high, jnp.zeros((8 - 2 * per, 128), F32)], axis=0)
    mine = jnp.concatenate([total[:base], tail], axis=0).astype(BF)
    return jnp.broadcast_to(mine[None], parts.shape)


def aux_rows(gathered, rows):
    vecs, aux = rows.shape
    groups = gathered.shape[0]
    columns = aux // 128
    tiles = (vecs // 8) * columns
    each = tiles // groups
    for t in range(tiles):
        r, q = divmod(t, columns)
        j, i = divmod(t, each)
        rows[8 * r : 8 * r + 8, 128 * q : 128 * q + 128] = gathered[j, 8 * i : 8 * i + 8, :]


def coupled_kernel(integrals, kept, gathered, other, own, rows, held, sems):
    ys, cs = lax.axis_size("y"), lax.axis_size("c")
    saved = kept.shape[0]
    share_rows = integrals.shape[0] // (ys * cs)
    y, c = lax.axis_index("y"), lax.axis_index("c")
    size = held.shape[1]
    copies = [
        pltpu.make_async_copy(integrals.at[pl.ds(saved + n * size, size)], held.at[n], sems.at[n])
        for n in range(held.shape[0])
    ]
    for copy in copies:
        copy.start()
    aux_rows(gathered, rows)
    a = rows[...]
    vecs = a.shape[0]
    gram = lax.dot_general(a, a, NT, preferred_element_type=F32)
    half = vecs // 2
    corner = jnp.concatenate([gram[:half], gram[half:, half:]], axis=1)
    strip = jnp.concatenate([corner[8 * i : 8 * i + 8] for i in range(half // 8)], axis=1).astype(BF)
    for n in range(ys):
        own[n, vecs:, :] = strip.astype(F32)
        other[n, vecs:, :] = strip

    def emit(first, source):
        block = lax.dot_general(a, source, NT, preferred_element_type=F32)
        for u in range(source.shape[0] // share_rows):
            n, half = divmod(first // share_rows + u, cs)
            to = lax.rem(n + ys - y, ys)
            piece = block[:, u * share_rows : (u + 1) * share_rows]

            @pl.when(c == half)
            def _():
                own[to, :vecs, :] = piece

            @pl.when(c != half)
            def _():
                other[to, :vecs, :] = piece.astype(BF)

    emit(0, kept[...])
    for n, copy in enumerate(copies):
        copy.wait()
        emit(saved + n * size, held[n])


def coupled(integrals, kept, gathered, vecs):
    pairs, aux = integrals.shape
    ys = lax.axis_size("y")
    shape = (ys, vecs + 8, pairs // (ys * lax.axis_size("c")))
    waits = 2
    return pl.pallas_call(
        coupled_kernel,
        out_shape=[
            jax.ShapeDtypeStruct(shape, BF),
            jax.ShapeDtypeStruct(shape, F32),
        ],
        in_specs=[HBM, VMEM, VMEM],
        out_specs=[VMEM, VMEM],
        scratch_shapes=[
            pltpu.VMEM((vecs, aux), BF),
            pltpu.VMEM((waits, (pairs - kept.shape[0]) // waits, aux), BF),
            pltpu.SemaphoreType.DMA((waits,)),
        ],
        compiler_params=pltpu.CompilerParams(vmem_limit_bytes=COUPLED_LIMIT),
        cost_estimate=pl.CostEstimate(flops=2 * pairs * aux * 256, bytes_accessed=2 * pairs * aux, transcendentals=0),
        name="coupled",
    )(integrals, kept, gathered)


def deal(own, other):
    total = own + other.astype(F32)
    return total[0], *[total[k].astype(BF) for k in range(1, own.shape[0])]


def sigma_kernel(total_pairs, stats, trial, gaps, kept, one, two, three, coupled_sum, rates, products, norms, grams):
    ys = 4
    y = lax.axis_index("y")
    vecs, rows = trial.shape
    for k, part in enumerate((kept, one, two, three)):
        grams[lax.rem(y + ys - k, ys)] = part[vecs:, :].astype(BF).astype(F32)
    strip = grams[0] + grams[1] + grams[2] + grams[3]
    half = vecs // 2
    lanes = half + vecs
    corner = jnp.concatenate([strip[:, lanes * i : lanes * i + lanes] for i in range(half // 8)], axis=0)
    turned = jnp.transpose(jnp.concatenate([corner, jnp.zeros((half, 128 - lanes), F32)], axis=1))
    lower = jnp.concatenate([turned[half:vecs], corner[:, vecs:]], axis=1)
    gram = jnp.concatenate([corner[:, :vecs], lower], axis=0)
    wide = stats[...]
    product = wide[:, :vecs] + 2.0 * gram
    products[...] = product
    r = lax.broadcasted_iota(jnp.int32, (vecs, vecs), 0)
    q = lax.broadcasted_iota(jnp.int32, (vecs, vecs), 1)
    diagonal = jnp.sum(jnp.where(r == q, product, 0.0), axis=1, keepdims=True)
    rayleigh = diagonal / total_pairs / (wide[:, vecs : vecs + 1] / total_pairs + epsilon)
    rates[...] = jnp.broadcast_to(rayleigh, rates.shape)
    block = kept[:vecs, :]
    for part in (one, two, three):
        block = block + part[:vecs, :].astype(F32)
    coupled_sum[...] = block
    x = trial[...]
    rest = gaps[...] * x + 2.0 * block - rayleigh * x
    sums = jnp.sum(rest * rest, axis=1, keepdims=True)
    line = jnp.sum(jnp.where(r == q, jnp.broadcast_to(sums, (vecs, vecs)), 0.0), axis=0, keepdims=True)
    norms[...] = jnp.concatenate([line, jnp.zeros_like(line)], axis=1)


def sigma_rows(total_pairs, stats, trial, gaps, parts):
    vecs, rows = trial.shape
    return pl.pallas_call(
        lambda *refs: sigma_kernel(total_pairs, *refs),
        out_shape=[
            jax.ShapeDtypeStruct((vecs, rows), F32),
            jax.ShapeDtypeStruct((vecs, rows), F32),
            jax.ShapeDtypeStruct((vecs, vecs), F32),
            jax.ShapeDtypeStruct((1, 128), F32),
        ],
        in_specs=[VMEM] * 7,
        out_specs=[VMEM] * 4,
        scratch_shapes=[pltpu.VMEM((4, 8, rows), F32)],
        compiler_params=pltpu.CompilerParams(vmem_limit_bytes=16 << 20),
        cost_estimate=pl.CostEstimate(flops=20 * trial.size, bytes_accessed=16 * trial.size, transcendentals=0),
        name="sigma_rows",
    )(stats, trial, gaps, *parts)


def finish_kernel(total_pairs, arrived, products, subspace, norms):
    subspace[...] = products[...] / total_pairs
    sums = jnp.sum(arrived[...], axis=0, keepdims=True)
    norms[...] = jnp.sqrt(sums / total_pairs + epsilon)[:, : norms.shape[1]]


def finish(total_pairs, arrived, products):
    return pl.pallas_call(
        lambda *refs: finish_kernel(total_pairs, *refs),
        out_shape=[jax.ShapeDtypeStruct(products.shape, F32), jax.ShapeDtypeStruct((1, products.shape[0]), F32)],
        in_specs=[VMEM] * 2,
        out_specs=[VMEM] * 2,
        compiler_params=pltpu.CompilerParams(vmem_limit_bytes=16 << 20),
        name="finish",
    )(arrived, products)


def exchange(value, axis):
    return lax.all_to_all(value, axis, 0, 0, tiled=True)


def shifted(value, axis, by):
    n = lax.axis_size(axis)
    return lax.ppermute(value, axis, [(i, (i + by) % n) for i in range(n)])


def local(integrals, energy_gaps, trial_vectors):
    pairs, vecs = trial_vectors.shape
    groups = lax.axis_size(PAIR)
    ys, cs = lax.axis_size("y"), lax.axis_size("c")
    total_pairs = float(pairs * groups)
    per = vecs // groups
    share_rows = pairs // (ys * cs)
    trial = trial_vectors.T
    gaps = energy_gaps.reshape(1, pairs)
    parts = totals(integrals, trial, gaps, groups)
    mine = share(exchange(parts, PAIR), per)
    first = (lax.axis_index("y") * cs + lax.axis_index("c")) * share_rows
    own_trial = lax.dynamic_slice_in_dim(trial, first, share_rows, 1)
    own_gaps = lax.dynamic_slice_in_dim(gaps, first, share_rows, 1)
    kept = lax.slice_in_dim(integrals, 0, pairs // ys, axis=0)
    mine, own_trial, own_gaps, kept = lax.optimization_barrier((mine, own_trial, own_gaps, kept))
    gathered = exchange(mine, PAIR)
    other, own = coupled(integrals, kept, gathered, vecs)
    arrived = shifted(other, "c", 1)
    mine, *sent = deal(own, arrived)
    far = shifted(sent[1], "y", 2)
    came = [shifted(sent[0], "y", 1), far, shifted(sent[2], "y", 3)]
    base = gathered.shape[1] - 8
    stats = gathered[:, base : base + per, :].astype(F32) + gathered[:, base + per : base + 2 * per, :].astype(F32)
    stats = stats.reshape(vecs, 128)
    coupled_sum, rates, products, norms = sigma_rows(total_pairs, stats, own_trial, own_gaps, [mine, *came])
    coupled_sum, own_trial, own_gaps = lax.optimization_barrier((coupled_sum, own_trial, own_gaps))
    sigma = own_gaps * own_trial + 2.0 * coupled_sum
    residuals = sigma - rates * own_trial
    norms = norms + shifted(norms, "c", 1)
    norms, sigma, residuals = lax.optimization_barrier((norms, sigma, residuals))
    everyone = ("z", "y", "x")
    copies = jnp.broadcast_to(norms, (lax.axis_size(everyone), 1, 128))
    arrived = exchange(copies, everyone).reshape(-1, 128)
    subspace, residual_norms = finish(total_pairs, arrived, products)
    residual_norms = residual_norms.reshape(vecs)
    return (sigma.T, subspace, residuals.T, residual_norms)


def solution(mesh):
    finer = Mesh(mesh.devices.reshape(8, 4, 4, 2), ALL)
    return jax.shard_map(
        local,
        mesh=finer,
        in_specs=(P(PAIR, AUX), P(PAIR), P(PAIR, None)),
        out_specs=(P(ALL, None), P(), P(ALL, None), P()),
        check_vma=False,
    )
```
